32 devices in a mesh: role: 2 (over x), grp: 2 (over y), tp: 8 (over z, core).
Axes of the slice: x: 2, y: 2, z: 4, core: 2. Of those that a mesh axis runs over, the one named last changes fastest.
Arguments:
- queries: bfloat16 [2, 8, 8192], P(None, None, ('grp', 'tp')), may hold values from -130 to 130
- step_token_keys: bfloat16 [2, 8, 1024], replicated, may hold values from -6 to 6
- step_token_values: bfloat16 [2, 8, 1024], replicated, may hold values from -6 to 6
- stored_key_cache: bfloat16 [8, 512, 1024], P(None, ('grp', 'tp')), may hold values from -6 to 6
- stored_value_cache: bfloat16 [8, 512, 1024], P(None, ('grp', 'tp')), may hold values from -6 to 6
- lengths: int32 [8], replicated, may hold values from 2 to 512
- wo_sides: bfloat16 [2, 8192, 8192], P('role', ('grp', 'tp')), may hold values from -1 to 1
- gain_sides: float32 [2, 8192], P('role', ('grp', 'tp')), may hold values from 0.5 to 1.5
- head: bfloat16 [8192, 64128], P(None, ('grp', 'tp')), may hold values from -8 to 8
- resid: bfloat16 [2, 8, 8192], P(None, None, ('grp', 'tp')), may hold values from -90 to 90
- actions: int32 [2, 8], replicated, may hold values from 0 to 64127
Outputs:
- log_probs: float32 [2, 8], P('role')
- normed: bfloat16 [2, 8, 8192], P('role', None, ('grp', 'tp'))
The draws below stay inside these ranges and needn't reach their ends.
All inputs are finite; a program needn't handle non-finite values.
Results may differ from the reference program's by a relative error of at most 0.017.
Values may be sent and summed in bfloat16 or wider, within the bound.
A program may use at most 128 MiB of HBM per device.

```python
import math
import jax
import jax.numpy as jnp
from jax import lax

D = 8192
QUERY_HEADS = 64
KEY_VALUE_HEADS = 8
HEAD_SIZE = 128
V = 64128
DECODED_ROWS = 8
DECODE_STEPS = 2
HD = 8192
CACHE_SLOTS = 512


def key_table(key):
    return jnp.clip(jax.random.normal(jax.random.fold_in(key, 11), (DECODED_ROWS, CACHE_SLOTS, KEY_VALUE_HEADS * HEAD_SIZE), jnp.float32), -6.0, 6.0)


def draw_stored_key_cache(key, part):
    base_offset = key_table(key)
    return base_offset.astype(jnp.bfloat16)


def draw_queries(key, part):
    drawn = jnp.clip(jax.random.normal(jax.random.fold_in(key, 23), (DECODE_STEPS, DECODED_ROWS, QUERY_HEADS * HEAD_SIZE), jnp.float32), -6.0, 6.0)
    return drawn.astype(jnp.bfloat16)


def draw_resid(key, part):
    noise = jnp.clip(jax.random.normal(jax.random.fold_in(key, 31), (DECODE_STEPS, DECODED_ROWS, D), jnp.float32), -6.0, 6.0)
    ramp = 0.5 + jnp.arange(D, dtype=jnp.float32) / D
    values = noise * ramp[None, None, :]
    return values.astype(jnp.bfloat16)


def draw_head(key, part):
    base_offset = jnp.clip(jax.random.normal(jax.random.fold_in(key, 41), (D, V), jnp.float32), -6.0, 6.0) * (3.0 / math.sqrt(D))
    base_offset = jnp.clip(base_offset, -8.0, 8.0)
    return base_offset.astype(jnp.bfloat16)


def plant(array, stream_key, smallest, high):
    longest = array.shape.index(max(array.shape))
    spots = []
    for shift in (0, 1):
        where = [jax.random.randint(jax.random.fold_in(stream_key, axis), (), 0, length) for axis, length in enumerate(array.shape)]
        where[longest] = (where[longest] + shift) % array.shape[longest]
        spots.append(tuple(where))
    return array.at[spots[0]].set(smallest).at[spots[1]].set(high)


def block_levels(own_key, dims, cuts, smallest, high):
    def one(position, blocks):
        heights = jax.random.uniform(jax.random.fold_in(jax.random.fold_in(own_key, 6), position), (blocks,), jnp.float32, smallest / len(cuts), high / len(cuts))
        return jnp.repeat(jnp.exp(heights), dims[position] // blocks).reshape((-1,) + (1,) * (len(dims) - position - 1))

    level = one(*cuts[0])
    for cut in cuts[1:]:
        level = level * one(*cut)
    return level


def scatter_about(own_key, extent, spread, reach, cuts=(), kind=jnp.bfloat16):
    entries = spread * jax.random.normal(own_key, extent, jnp.float32)
    if cuts:
        entries = entries * block_levels(own_key, extent, cuts, -0.22, 0.18)
    return jnp.clip(entries, -reach, reach).astype(kind)


def setup_inputs(seed: int = 0) -> dict:
    splits = jax.random.split(jax.random.key(seed), 12)
    return {
        "queries": draw_queries(jax.random.fold_in(splits[11], 71), 0),
        "step_token_keys": scatter_about(splits[1], (DECODE_STEPS, DECODED_ROWS, KEY_VALUE_HEADS * HEAD_SIZE), 1.0, 6.0),
        "step_token_values": scatter_about(splits[2], (DECODE_STEPS, DECODED_ROWS, KEY_VALUE_HEADS * HEAD_SIZE), 1.0, 6.0),
        "stored_key_cache": draw_stored_key_cache(jax.random.fold_in(splits[11], 71), 0),
        "stored_value_cache": scatter_about(splits[4], (DECODED_ROWS, CACHE_SLOTS, KEY_VALUE_HEADS * HEAD_SIZE), 1.0, 6.0, ((1, 16),)),
        "lengths": plant(jax.random.randint(splits[5], (DECODED_ROWS,), 2, CACHE_SLOTS + 1), jax.random.fold_in(splits[5], 1), 2, CACHE_SLOTS).astype(jnp.int32),
        "wo_sides": scatter_about(splits[6], (2, HD, D), (max(HD // 256, 1)) ** -0.5, 1.0, ((0, 2), (1, 16))),
        "gain_sides": jnp.clip(1.0 + 0.1 * jax.random.normal(splits[7], (2, D), jnp.float32), 0.5, 1.5),
        "head": draw_head(jax.random.fold_in(splits[11], 71), 0),
        "resid": draw_resid(jax.random.fold_in(splits[11], 71), 0),
        "actions": plant(jax.random.randint(splits[10], (DECODE_STEPS, DECODED_ROWS), 0, V), jax.random.fold_in(splits[10], 1), 0, V - 1).astype(jnp.int32),
    }


def reference(queries, step_token_keys, step_token_values, stored_key_cache, stored_value_cache, lengths, wo_sides, gain_sides, head, resid, actions):
    count_of_rows = lengths.shape[0]
    query_group_width = QUERY_HEADS // KEY_VALUE_HEADS
    logit_scale = 1.0 / math.sqrt(HEAD_SIZE)
    positions = jnp.arange(CACHE_SLOTS, dtype=jnp.int32)
    valid = positions[None, :] < lengths[:, None]
    masking = valid[:, None, None, :]
    prior_keys = stored_key_cache.astype(jnp.float32).reshape(count_of_rows, CACHE_SLOTS, KEY_VALUE_HEADS, HEAD_SIZE)
    prior_values = stored_value_cache.astype(jnp.float32).reshape(count_of_rows, CACHE_SLOTS, KEY_VALUE_HEADS, HEAD_SIZE)
    vocab_ids = jnp.arange(V, dtype=jnp.int32)
    prob_list = []
    normed_list = []
    for decode_index in range(DECODE_STEPS):
        version = 1 - decode_index
        current_query = queries[decode_index].astype(jnp.float32).reshape(count_of_rows, KEY_VALUE_HEADS, query_group_width, HEAD_SIZE) * logit_scale
        scores = jnp.einsum('rkgd,rskd->rkgs', current_query, prior_keys)
        scores = jnp.where(masking, scores, -1e+30)
        incoming_keys = step_token_keys[:decode_index + 1].astype(jnp.float32).reshape(decode_index + 1, count_of_rows, KEY_VALUE_HEADS, HEAD_SIZE)
        incoming_values = step_token_values[:decode_index + 1].astype(jnp.float32).reshape(decode_index + 1, count_of_rows, KEY_VALUE_HEADS, HEAD_SIZE)
        fresh_scores = jnp.einsum('rkgd,trkd->rkgt', current_query, incoming_keys)
        highest = jnp.maximum(lax.optimization_barrier(jnp.max(scores, axis=-1)), lax.optimization_barrier(jnp.max(fresh_scores, axis=-1)))
        cache_probs = jnp.exp(scores - highest[..., None]) * masking
        fresh_probs = jnp.exp(fresh_scores - highest[..., None])
        totals = lax.optimization_barrier(jnp.sum(cache_probs, axis=-1)) + lax.optimization_barrier(jnp.sum(fresh_probs, axis=-1))
        weighted = jnp.einsum('rkgs,rskd->rkgd', cache_probs, prior_values) + jnp.einsum('rkgt,trkd->rkgd', fresh_probs, incoming_values)
        attended = (weighted / totals[..., None]).reshape(count_of_rows, QUERY_HEADS * HEAD_SIZE).astype(jnp.bfloat16)
        state = resid[decode_index].astype(jnp.float32) + jnp.dot(attended, wo_sides[version], preferred_element_type=jnp.float32)
        mean_square = lax.optimization_barrier(jnp.mean(state * state, axis=-1, keepdims=True))
        normed_now = (state * jax.lax.rsqrt(mean_square + 1e-05) * gain_sides[version][None, :]).astype(jnp.bfloat16)
        logits = jnp.dot(normed_now, head, preferred_element_type=jnp.float32)
        largest = lax.optimization_barrier(jnp.max(logits, axis=-1))
        exp_sum = lax.optimization_barrier(jnp.sum(jnp.exp(logits - largest[:, None]), axis=-1))
        is_target = vocab_ids[None, :] == actions[decode_index][:, None]
        target = lax.optimization_barrier(jnp.sum(jnp.where(is_target, logits, 0.0), axis=-1))
        prob_list.append(target - largest - jnp.log(exp_sum))
        normed_list.append(normed_now)
    return (jnp.stack(prob_list), jnp.stack(normed_list))
```

```python
import math

import jax
import jax.numpy as jnp
from jax import lax
from jax.sharding import PartitionSpec as P

D = 8192
QUERY_HEADS = 64
KEY_VALUE_HEADS = 8
HEAD_SIZE = 128
DECODE_STEPS = 2


def swap_sides(value):
    return lax.ppermute(value, "role", [(0, 1), (1, 0)])


def on_device(
    queries,
    step_token_keys,
    step_token_values,
    stored_key_cache,
    stored_value_cache,
    lengths,
    wo_sides,
    gain_sides,
    head,
    resid,
    actions,
):
    both = ("grp", "tp")
    place = lax.axis_index(both)
    step = 1 - lax.axis_index("role")
    count_of_rows = lengths.shape[0]
    shard_length = stored_key_cache.shape[1]
    query_group_width = QUERY_HEADS // KEY_VALUE_HEADS
    logit_scale = 1.0 / math.sqrt(HEAD_SIZE)
    query_matrix = lax.all_gather(
        lax.dynamic_index_in_dim(queries, step, 0, keepdims=False), both, axis=1, tiled=True
    )
    positions = place * shard_length + jnp.arange(shard_length, dtype=jnp.int32)
    valid = positions[None, :] < lengths[:, None]
    masking = valid[:, None, None, :]
    cache_shape = (count_of_rows, shard_length, KEY_VALUE_HEADS, HEAD_SIZE)
    prior_keys = stored_key_cache.reshape(cache_shape)
    prior_values = stored_value_cache.reshape(cache_shape)
    step_shape = (DECODE_STEPS, count_of_rows, KEY_VALUE_HEADS, HEAD_SIZE)
    incoming_keys = step_token_keys.astype(jnp.float32).reshape(step_shape)
    incoming_values = step_token_values.astype(jnp.float32).reshape(step_shape)
    current_query = query_matrix.reshape(
        count_of_rows, KEY_VALUE_HEADS, query_group_width, HEAD_SIZE
    )
    scores = (
        jnp.einsum("rkgd,rskd->rkgs", current_query, prior_keys, preferred_element_type=jnp.float32)
        * logit_scale
    )
    scores = jnp.where(masking, scores, -1e30)
    fresh_live = jnp.arange(DECODE_STEPS, dtype=jnp.int32) <= step
    fresh_scores = (
        jnp.einsum("rkgd,trkd->rkgt", current_query.astype(jnp.float32), incoming_keys)
        * logit_scale
    )
    fresh_scores = jnp.where(fresh_live, fresh_scores, -1e30)
    fresh_highest = jnp.max(fresh_scores, axis=-1)
    overall = lax.pmax(jnp.maximum(jnp.max(scores, axis=-1), fresh_highest), both)
    cache_probs = jnp.exp(scores - overall[..., None]) * masking
    fresh_probs = jnp.exp(fresh_scores - overall[..., None]) * fresh_live
    fresh_probs = fresh_probs * (place == 0)
    totals = jnp.sum(cache_probs, axis=-1) + jnp.sum(fresh_probs, axis=-1)
    weighted = jnp.einsum(
        "rkgs,rskd->rkgd", cache_probs, prior_values.astype(jnp.float32)
    ) + jnp.einsum("rkgt,trkd->rkgd", fresh_probs, incoming_values)
    features = QUERY_HEADS * HEAD_SIZE
    mixed = lax.psum_scatter(
        weighted.reshape(count_of_rows, features), both, scatter_dimension=1, tiled=True
    )
    totals = lax.psum(totals.reshape(count_of_rows, QUERY_HEADS), both)
    feature_rows = wo_sides.shape[1]
    own_heads = (place * feature_rows + jnp.arange(feature_rows)) // HEAD_SIZE
    own_part = (mixed / jnp.take(totals, own_heads, axis=1)).astype(jnp.bfloat16)
    branch_out = lax.psum_scatter(
        jnp.dot(own_part, wo_sides[0], preferred_element_type=jnp.float32),
        both,
        scatter_dimension=1,
        tiled=True,
    )
    resid_now = lax.dynamic_index_in_dim(resid, step, 0, keepdims=False)
    state = resid_now.astype(jnp.float32) + branch_out
    square_sum = lax.psum(jnp.sum(state * state, axis=-1), both)
    normed_now = (
        state * lax.rsqrt(square_sum[:, None] / D + 1e-05) * gain_sides[0][None, :]
    ).astype(jnp.bfloat16)
    logits = jnp.dot(
        lax.all_gather(normed_now, both, axis=1, tiled=True),
        head,
        preferred_element_type=jnp.float32,
    )
    local_highest = jnp.max(logits, axis=-1)
    action_now = lax.dynamic_index_in_dim(actions, step, 0, keepdims=False)
    head_width = head.shape[1]
    vocab_ids = place * head_width + jnp.arange(head_width, dtype=jnp.int32)
    is_target = vocab_ids[None, :] == action_now[:, None]
    target = jnp.sum(jnp.where(is_target, logits, 0.0), axis=-1)
    exp_sum = jnp.sum(jnp.exp(logits - local_highest[:, None]), axis=-1)
    parts = lax.all_gather(jnp.stack([local_highest, exp_sum, target]), both)
    largest = jnp.max(parts[:, 0], axis=0)
    exp_sum = jnp.sum(parts[:, 1] * jnp.exp(parts[:, 0] - largest[None]), axis=0)
    prob_now = jnp.sum(parts[:, 2], axis=0) - largest - jnp.log(exp_sum)
    return (swap_sides(prob_now)[None], swap_sides(normed_now)[None])


def solution(mesh):
    in_specs = (
        P(None, None, ("grp", "tp")),
        P(),
        P(),
        P(None, ("grp", "tp"), None),
        P(None, ("grp", "tp"), None),
        P(),
        P("role", ("grp", "tp"), None),
        P("role", ("grp", "tp")),
        P(None, ("grp", "tp")),
        P(None, None, ("grp", "tp")),
        P(),
    )
    out_specs = (P("role", None), P("role", None, ("grp", "tp")))
    return jax.shard_map(
        on_device, mesh=mesh, in_specs=in_specs, out_specs=out_specs, check_vma=False
    )
```

```python
import functools
import math

import jax
import jax.numpy as jnp
from jax import lax
from jax.experimental import pallas as pl
from jax.experimental.pallas import tpu as pltpu
from jax.sharding import PartitionSpec as P

D = 8192
QUERY_HEADS = 64
KEY_VALUE_HEADS = 8
HEAD_SIZE = 128
DECODE_STEPS = 2


def swap_sides(value):
    return lax.ppermute(value, "role", [(0, 1), (1, 0)])


def plain(
    queries,
    step_token_keys,
    step_token_values,
    stored_key_cache,
    stored_value_cache,
    lengths,
    wo_sides,
    gain_sides,
    head,
    resid,
    actions,
):
    both = ("grp", "tp")
    place = lax.axis_index(both)
    step = 1 - lax.axis_index("role")
    count_of_rows = lengths.shape[0]
    shard_length = stored_key_cache.shape[1]
    query_group_width = QUERY_HEADS // KEY_VALUE_HEADS
    logit_scale = 1.0 / math.sqrt(HEAD_SIZE)
    query_matrix = lax.all_gather(
        lax.dynamic_index_in_dim(queries, step, 0, keepdims=False), both, axis=1, tiled=True
    )
    positions = place * shard_length + jnp.arange(shard_length, dtype=jnp.int32)
    valid = positions[None, :] < lengths[:, None]
    masking = valid[:, None, None, :]
    cache_shape = (count_of_rows, shard_length, KEY_VALUE_HEADS, HEAD_SIZE)
    prior_keys = stored_key_cache.reshape(cache_shape)
    prior_values = stored_value_cache.reshape(cache_shape)
    step_shape = (DECODE_STEPS, count_of_rows, KEY_VALUE_HEADS, HEAD_SIZE)
    incoming_keys = step_token_keys.astype(jnp.float32).reshape(step_shape)
    incoming_values = step_token_values.astype(jnp.float32).reshape(step_shape)
    current_query = query_matrix.reshape(
        count_of_rows, KEY_VALUE_HEADS, query_group_width, HEAD_SIZE
    )
    scores = (
        jnp.einsum("rkgd,rskd->rkgs", current_query, prior_keys, preferred_element_type=jnp.float32)
        * logit_scale
    )
    scores = jnp.where(masking, scores, -1e30)
    fresh_live = jnp.arange(DECODE_STEPS, dtype=jnp.int32) <= step
    fresh_scores = (
        jnp.einsum("rkgd,trkd->rkgt", current_query.astype(jnp.float32), incoming_keys)
        * logit_scale
    )
    fresh_scores = jnp.where(fresh_live, fresh_scores, -1e30)
    fresh_highest = jnp.max(fresh_scores, axis=-1)
    overall = lax.pmax(jnp.maximum(jnp.max(scores, axis=-1), fresh_highest), both)
    cache_probs = jnp.exp(scores - overall[..., None]) * masking
    fresh_probs = jnp.exp(fresh_scores - overall[..., None]) * fresh_live
    fresh_probs = fresh_probs * (place == 0)
    totals = jnp.sum(cache_probs, axis=-1) + jnp.sum(fresh_probs, axis=-1)
    weighted = jnp.einsum(
        "rkgs,rskd->rkgd", cache_probs, prior_values.astype(jnp.float32)
    ) + jnp.einsum("rkgt,trkd->rkgd", fresh_probs, incoming_values)
    features = QUERY_HEADS * HEAD_SIZE
    mixed = lax.psum_scatter(
        weighted.reshape(count_of_rows, features), both, scatter_dimension=1, tiled=True
    )
    totals = lax.psum(totals.reshape(count_of_rows, QUERY_HEADS), both)
    feature_rows = wo_sides.shape[1]
    own_heads = (place * feature_rows + jnp.arange(feature_rows)) // HEAD_SIZE
    own_part = (mixed / jnp.take(totals, own_heads, axis=1)).astype(jnp.bfloat16)
    branch_out = lax.psum_scatter(
        jnp.dot(own_part, wo_sides[0], preferred_element_type=jnp.float32),
        both,
        scatter_dimension=1,
        tiled=True,
    )
    resid_now = lax.dynamic_index_in_dim(resid, step, 0, keepdims=False)
    state = resid_now.astype(jnp.float32) + branch_out
    square_sum = lax.psum(jnp.sum(state * state, axis=-1), both)
    normed_now = (
        state * lax.rsqrt(square_sum[:, None] / D + 1e-05) * gain_sides[0][None, :]
    ).astype(jnp.bfloat16)
    logits = jnp.dot(
        lax.all_gather(normed_now, both, axis=1, tiled=True),
        head,
        preferred_element_type=jnp.float32,
    )
    local_highest = jnp.max(logits, axis=-1)
    action_now = lax.dynamic_index_in_dim(actions, step, 0, keepdims=False)
    head_width = head.shape[1]
    vocab_ids = place * head_width + jnp.arange(head_width, dtype=jnp.int32)
    is_target = vocab_ids[None, :] == action_now[:, None]
    target = jnp.sum(jnp.where(is_target, logits, 0.0), axis=-1)
    exp_sum = jnp.sum(jnp.exp(logits - local_highest[:, None]), axis=-1)
    parts = lax.all_gather(jnp.stack([local_highest, exp_sum, target]), both)
    largest = jnp.max(parts[:, 0], axis=0)
    exp_sum = jnp.sum(parts[:, 1] * jnp.exp(parts[:, 0] - largest[None]), axis=0)
    prob_now = jnp.sum(parts[:, 2], axis=0) - largest - jnp.log(exp_sum)
    return (swap_sides(prob_now)[None], swap_sides(normed_now)[None])


LOW = -1e30
TILE = 512
MESH = pl.DeviceIdType.MESH


def fused_kernel(
    n,
    tp,
    queries,
    token_keys,
    token_values,
    keys,
    values,
    lengths,
    gain,
    resid,
    actions,
    wo,
    head,
    log_probs,
    normed,
    wo_buf,
    head_buf,
    q_all,
    b_send,
    b_recv,
    c_send,
    c_recv,
    d_send,
    d_recv,
    x_send,
    x_recv,
    s_send,
    s_recv,
    x_rows,
    y_keep,
    y_send,
    y_recv,
    e_send,
    e_recv,
    wo_sem,
    head_sems,
    q_ss,
    q_rs,
    b_ss,
    b_rs,
    c_ss,
    c_rs,
    d_ss,
    d_rs,
    x_sem,
    s_ss,
    s_rs,
    y_ss,
    y_rs,
    e_ss,
    e_rs,
):
    role = lax.axis_index("role")
    me = lax.axis_index("grp") * tp + lax.axis_index("tp")
    step = 1 - role
    half = n // 2
    rows = lengths.shape[0]
    shard = keys.shape[1]
    width = resid.shape[2]
    own_heads = width // HEAD_SIZE
    group = QUERY_HEADS // KEY_VALUE_HEADS
    slots = rows * shard
    depth = head_buf.shape[1]
    vocab = head.shape[0]
    full = vocab // TILE
    tail = vocab - full * TILE
    tiles = y_keep.shape[0]
    scale = 1.0 / math.sqrt(HEAD_SIZE)
    f32 = jnp.float32
    bf16 = jnp.bfloat16

    def device(side, place):
        return (side, place // tp, place % tp)

    def remote(src, dst, ss, rs, side, place):
        return pltpu.make_async_remote_copy(
            src_ref=src,
            dst_ref=dst,
            send_sem=ss,
            recv_sem=rs,
            device_id=device(side, place),
            device_id_type=MESH,
        )

    wo_copy = pltpu.make_async_copy(wo.at[0], wo_buf, wo_sem)
    wo_copy.start()

    def head_copy(first, size, sem):
        return pltpu.make_async_copy(
            head.at[pl.ds(first, size), pl.ds(pl.multiple_of(role * depth, 128), depth)],
            head_buf.at[pl.ds(first, size), :],
            sem,
        )

    @pl.loop(0, full)
    def _(j):
        head_copy(pl.multiple_of(j * TILE, TILE), TILE, head_sems.at[j]).start()

    if tail:
        head_copy(full * TILE, tail, head_sems.at[full]).start()

    barrier = pltpu.get_barrier_semaphore()

    @pl.loop(1, 2 * n)
    def _(i):
        other = (role * n + me + i) % (2 * n)
        pl.semaphore_signal(
            barrier, inc=1, device_id=device(other // n, other % n), device_id_type=MESH
        )

    pl.semaphore_wait(barrier, 2 * n - 1)

    @pl.loop(1, n)
    def _(i):
        to = (me + i) % n
        remote(queries.at[step], q_all.at[me], q_ss.at[i], q_rs.at[me], role, to).start()

    q_all[me] = queries[step]

    row_ids = lax.broadcasted_iota(jnp.int32, (group * rows, slots), 0) % rows
    col_ids = lax.broadcasted_iota(jnp.int32, (group * rows, slots), 1)
    limit = jnp.zeros((group * rows, slots), jnp.int32)
    for b in range(rows):
        limit = jnp.where(row_ids == b, lengths[b], limit)
    place_ids = me * shard + col_ids % shard
    live = (col_ids // shard == row_ids) & (place_ids < limit)

    @pl.loop(1, n)
    def _(i):
        src = (me + i) % n
        remote(queries.at[step], q_all.at[src], q_ss.at[i], q_rs.at[src], role, me).wait_recv()

    lane = lax.broadcasted_iota(jnp.int32, (rows, HEAD_SIZE), 1)
    per_group = group // own_heads
    for k in range(KEY_VALUE_HEADS):
        lanes = slice(k * HEAD_SIZE, (k + 1) * HEAD_SIZE)
        query = jnp.concatenate(
            [
                q_all[
                    k * per_group + h // own_heads,
                    :,
                    (h % own_heads) * HEAD_SIZE : (h % own_heads + 1) * HEAD_SIZE,
                ].astype(f32)
                for h in range(group)
            ],
            axis=0,
        ).astype(bf16)
        key = keys[:, :, lanes].reshape(slots, HEAD_SIZE)
        value = values[:, :, lanes].reshape(slots, HEAD_SIZE)
        scores = (
            lax.dot_general(query, key, (((1,), (1,)), ((), ())), preferred_element_type=f32)
            * scale
        )
        scores = jnp.where(live, scores, LOW)
        top = jnp.max(scores, axis=1, keepdims=True).astype(bf16).astype(f32)
        probs = jnp.where(live, jnp.exp(scores - top), 0.0).astype(bf16)
        total = jnp.sum(probs.astype(f32), axis=1, keepdims=True)
        total_high = total.astype(bf16).astype(f32)
        total_low = total - total_high
        weighted = jnp.dot(probs, value, preferred_element_type=f32)
        for part in range(per_group):
            to = k * per_group + part
            stats = jnp.zeros((rows, HEAD_SIZE), f32)
            for j in range(own_heads):
                at = (part * own_heads + j) * rows
                stats = jnp.where(lane == j, top[at : at + rows], stats)
                stats = jnp.where(lane == own_heads + j, total_high[at : at + rows], stats)
                stats = jnp.where(lane == 2 * own_heads + j, total_low[at : at + rows], stats)
            first = part * own_heads * rows
            b_send[to] = jnp.concatenate(
                [weighted[first : first + own_heads * rows], stats, jnp.zeros_like(stats)], axis=0
            ).astype(bf16)

    @pl.loop(1, n)
    def _(i):
        to = (me + i) % n
        remote(b_send.at[to], b_recv.at[me], b_ss.at[i], b_rs.at[me], role, to).start()

    b_recv[me] = b_send[me]

    kv_lanes = pl.ds(pl.multiple_of((me // per_group) * HEAD_SIZE, HEAD_SIZE), HEAD_SIZE)
    own_query = queries[step].astype(f32)
    fresh = []
    fresh_values = []
    for u in range(DECODE_STEPS):
        fresh_key = token_keys[u, :, kv_lanes].astype(f32)
        fresh_values.append(token_values[u, :, kv_lanes].astype(f32))
        fresh.append(
            [
                jnp.where(
                    u <= step,
                    jnp.sum(
                        own_query[:, j * HEAD_SIZE : (j + 1) * HEAD_SIZE] * fresh_key,
                        axis=1,
                        keepdims=True,
                    )
                    * scale,
                    LOW,
                )
                for j in range(own_heads)
            ]
        )

    @pl.loop(1, n)
    def _(i):
        src = (me + i) % n
        remote(b_send.at[src], b_recv.at[src], b_ss.at[i], b_rs.at[src], role, me).wait_recv()

    stat_rows = slice(own_heads * rows, own_heads * rows + 16)
    stats = [b_recv[s, stat_rows, :].astype(f32)[:rows] for s in range(n)]
    top = functools.reduce(jnp.maximum, stats)
    tops = [
        functools.reduce(
            jnp.maximum, [fresh[u][j] for u in range(DECODE_STEPS)], top[:, j : j + 1]
        )
        for j in range(own_heads)
    ]
    numerator = [jnp.zeros((rows, HEAD_SIZE), f32) for _ in range(own_heads)]
    denominator = [jnp.zeros((rows, 1), f32) for _ in range(own_heads)]
    for j in range(own_heads):
        for u in range(DECODE_STEPS):
            weight = jnp.where(u <= step, jnp.exp(fresh[u][j] - tops[j]), 0.0)
            numerator[j] += weight * fresh_values[u]
            denominator[j] += weight
    for s in range(n):
        part = b_recv[s, : own_heads * rows, :].astype(f32)
        for j in range(own_heads):
            factor = jnp.exp(stats[s][:, j : j + 1] - tops[j])
            numerator[j] += factor * part[j * rows : (j + 1) * rows]
            at = own_heads + j
            denominator[j] += factor * (
                stats[s][:, at : at + 1] + stats[s][:, at + own_heads : at + own_heads + 1]
            )
    attended = jnp.concatenate(
        [numerator[j] / denominator[j] for j in range(own_heads)], axis=1
    ).astype(bf16)

    wo_copy.wait()

    def project(to):
        return jnp.dot(
            attended,
            wo_buf[:, pl.ds(pl.multiple_of(to * width, 128), width)],
            preferred_element_type=f32,
        )

    @pl.loop(1, n)
    def _(i):
        to = (me + i) % n
        c_send[to] = project(to).astype(bf16)
        remote(c_send.at[to], c_recv.at[me], c_ss.at[i], c_rs.at[me], role, to).start()

    c_recv[me] = jnp.zeros((rows, width), bf16)
    state = resid[step].astype(f32) + project(me)

    @pl.loop(1, n)
    def _(i):
        src = (me + i) % n
        remote(c_send.at[src], c_recv.at[src], c_ss.at[i], c_rs.at[src], role, me).wait_recv()

    for s in range(n):
        state += c_recv[s].astype(f32)

    x = state * gain[...]
    d_send[...] = x.astype(bf16)
    x_send[...] = x
    s_send[...] = jnp.broadcast_to(jnp.sum(state * state, axis=1, keepdims=True), (rows, HEAD_SIZE))
    target_role = me // half
    own_slot = role * half + me % half

    @pl.when(target_role != role)
    def _():
        remote(
            d_send, d_recv.at[own_slot], d_ss.at[0], d_rs.at[own_slot], target_role, me
        ).start()

    @pl.when(target_role == role)
    def _():
        d_recv[own_slot] = d_send[...]

    @pl.loop(1, n)
    def _(i):
        to = (me + i) % n
        remote(
            d_send, d_recv.at[own_slot], d_ss.at[i], d_rs.at[own_slot], target_role, to
        ).start()

    @pl.loop(0, n)
    def _(i):
        to = (me + i) % n
        remote(s_send, s_recv.at[me], s_ss.at[i], s_rs.at[me], 1 - role, to).start()

    remote(x_send, x_recv, x_sem.at[0], x_sem.at[1], 1 - role, me).start()

    @pl.loop(0, n)
    def _(slot):
        mine = (slot // half == role) & (role * half + slot % half == me)

        @pl.when(jnp.logical_not(mine))
        def _():
            remote(d_send, d_recv.at[slot], d_ss.at[0], d_rs.at[slot], role, me).wait_recv()

    for f in range(half):
        x_rows[:, f * width : (f + 1) * width] = jnp.concatenate(
            [d_recv[half + f].astype(f32), d_recv[f].astype(f32)], axis=0
        ).astype(bf16)

    def vocab_dot(block):
        return lax.dot_general(
            x_rows[...], block, (((1,), (1,)), ((), ())), preferred_element_type=f32
        )

    def y_copy(j):
        return remote(y_send.at[j], y_recv.at[j], y_ss.at[j], y_rs.at[j], 1 - role, me)

    @pl.loop(0, full)
    def _(j):
        first = pl.multiple_of(j * TILE, TILE)
        head_copy(first, TILE, head_sems.at[j]).wait()
        y = vocab_dot(head_buf[pl.ds(first, TILE), :])
        y_keep[j] = jnp.where(role == 0, y[:rows], y[rows:])
        y_send[j] = jnp.where(role == 0, y[rows:], y[:rows])
        y_copy(j).start()

    if tail:
        head_copy(full * TILE, tail, head_sems.at[full]).wait()
        y = vocab_dot(head_buf[full * TILE :, :])
        y_keep[full] = jnp.zeros((rows, TILE), f32)
        y_send[full] = jnp.zeros((rows, TILE), f32)
        y_keep[full, :, :tail] = jnp.where(role == 0, y[:rows], y[rows:])
        y_send[full, :, :tail] = jnp.where(role == 0, y[rows:], y[:rows])
        y_copy(full).start()

    @pl.loop(0, n)
    def _(s):
        remote(s_send, s_recv.at[s], s_ss.at[s], s_rs.at[s], role, me).wait_recv()

    square_sum = jnp.zeros((rows, HEAD_SIZE), f32)
    for s in range(n):
        square_sum += s_recv[s]
    inverse = lax.rsqrt(square_sum / (n * width) + 1e-05)[:, :1]
    remote(x_send, x_recv, x_sem.at[0], x_sem.at[1], role, me).wait_recv()
    normed[0] = (x_recv[...] * inverse).astype(bf16)

    action_rows = lax.broadcasted_iota(jnp.int32, (rows, 1), 0)
    action = jnp.zeros((rows, 1), jnp.int32)
    for b in range(rows):
        action = jnp.where(action_rows == b, actions[role, b], action)
    tile_ids = lax.broadcasted_iota(jnp.int32, (rows, TILE), 1)
    logits = []
    for j in range(tiles):
        y_copy(j).wait_recv()
        tile = (y_keep[j] + y_recv[j]) * inverse
        if j == full:
            tile = jnp.where(tile_ids < tail, tile, LOW)
        logits.append(tile)
    largest = jnp.max(functools.reduce(jnp.maximum, logits), axis=1, keepdims=True)
    exp_sum = jnp.zeros((rows, TILE), f32)
    target = jnp.zeros((rows, TILE), f32)
    for j in range(tiles):
        exp_sum += jnp.exp(logits[j] - largest)
        here = tile_ids + j * TILE == action - me * vocab
        if j == full:
            here = here & (tile_ids < tail)
        target += jnp.where(here, logits[j], 0.0)
    exp_sum = jnp.sum(exp_sum, axis=1, keepdims=True)
    target = jnp.sum(target, axis=1, keepdims=True)
    e_send[...] = jnp.where(lane == 0, largest, jnp.where(lane == 1, exp_sum, target))

    @pl.loop(1, n)
    def _(i):
        to = (me + i) % n
        remote(e_send, e_recv.at[me], e_ss.at[i], e_rs.at[me], role, to).start()

    e_recv[me] = e_send[...]

    @pl.loop(1, n)
    def _(i):
        src = (me + i) % n
        remote(e_send, e_recv.at[src], e_ss.at[i], e_rs.at[src], role, me).wait_recv()

    top = functools.reduce(jnp.maximum, [e_recv[s] for s in range(n)])[:, :1]
    exp_sum = jnp.zeros((rows, 1), f32)
    target = jnp.zeros((rows, 1), f32)
    for s in range(n):
        got = e_recv[s]
        exp_sum += got[:, 1:2] * jnp.exp(got[:, :1] - top)
        target += got[:, 2:3]
    result = jnp.broadcast_to(target - top - jnp.log(exp_sum), (rows, HEAD_SIZE))
    diagonal = lax.broadcasted_iota(jnp.int32, (rows, HEAD_SIZE), 0) == lane
    log_probs[...] = jnp.sum(jnp.where(diagonal, result, 0.0), axis=0, keepdims=True)[:, :rows]

    @pl.loop(1, n)
    def _(i):
        to = (me + i) % n
        remote(queries.at[step], q_all.at[me], q_ss.at[i], q_rs.at[me], role, to).wait_send()
        remote(b_send.at[to], b_recv.at[me], b_ss.at[i], b_rs.at[me], role, to).wait_send()
        remote(c_send.at[to], c_recv.at[me], c_ss.at[i], c_rs.at[me], role, to).wait_send()
        remote(
            d_send, d_recv.at[own_slot], d_ss.at[i], d_rs.at[own_slot], target_role, to
        ).wait_send()
        remote(e_send, e_recv.at[me], e_ss.at[i], e_rs.at[me], role, to).wait_send()

    @pl.when(target_role != role)
    def _():
        remote(
            d_send, d_recv.at[own_slot], d_ss.at[0], d_rs.at[own_slot], target_role, me
        ).wait_send()

    @pl.loop(0, n)
    def _(i):
        remote(s_send, s_recv.at[me], s_ss.at[i], s_rs.at[me], 1 - role, me).wait_send()

    remote(x_send, x_recv, x_sem.at[0], x_sem.at[1], 1 - role, me).wait_send()
    for j in range(tiles):
        y_copy(j).wait_send()


def fused(
    queries,
    step_token_keys,
    step_token_values,
    stored_key_cache,
    stored_value_cache,
    lengths,
    wo_sides,
    gain_sides,
    head,
    resid,
    actions,
):
    tp = lax.axis_size("tp")
    n = lax.axis_size("grp") * tp
    rows = lengths.shape[0]
    width = resid.shape[2]
    heads = width // HEAD_SIZE
    depth = head.shape[0] // 2
    tiles = -(-head.shape[1] // TILE)
    bf16, f32 = jnp.bfloat16, jnp.float32
    vmem = pl.BlockSpec(memory_space=pltpu.VMEM)
    smem = pl.BlockSpec(memory_space=pltpu.SMEM)
    hbm = pl.BlockSpec(memory_space=pl.ANY)
    message = heads * rows + 2 * rows
    dma = pltpu.SemaphoreType.DMA
    return pl.pallas_call(
        functools.partial(fused_kernel, n, tp),
        out_shape=(
            jax.ShapeDtypeStruct((1, rows), f32),
            jax.ShapeDtypeStruct((1, rows, width), bf16),
        ),
        in_specs=[vmem, vmem, vmem, vmem, vmem, smem, vmem, vmem, smem, hbm, hbm],
        out_specs=(vmem, vmem),
        scratch_shapes=[
            pltpu.VMEM(wo_sides.shape[1:], bf16),
            pltpu.VMEM((head.shape[1], depth), bf16),
            pltpu.VMEM((n, rows, width), bf16),
            pltpu.VMEM((n, message, HEAD_SIZE), bf16),
            pltpu.VMEM((n, message, HEAD_SIZE), bf16),
            pltpu.VMEM((n, rows, width), bf16),
            pltpu.VMEM((n, rows, width), bf16),
            pltpu.VMEM((rows, width), bf16),
            pltpu.VMEM((n, rows, width), bf16),
            pltpu.VMEM((rows, width), f32),
            pltpu.VMEM((rows, width), f32),
            pltpu.VMEM((rows, HEAD_SIZE), f32),
            pltpu.VMEM((n, rows, HEAD_SIZE), f32),
            pltpu.VMEM((2 * rows, depth), bf16),
            pltpu.VMEM((tiles, rows, TILE), f32),
            pltpu.VMEM((tiles, rows, TILE), f32),
            pltpu.VMEM((tiles, rows, TILE), f32),
            pltpu.VMEM((rows, HEAD_SIZE), f32),
            pltpu.VMEM((n, rows, HEAD_SIZE), f32),
            dma,
            dma((tiles,)),
            dma((n,)),
            dma((n,)),
            dma((n,)),
            dma((n,)),
            dma((n,)),
            dma((n,)),
            dma((n,)),
            dma((n,)),
            dma((2,)),
            dma((n,)),
            dma((n,)),
            dma((tiles,)),
            dma((tiles,)),
            dma((n,)),
            dma((n,)),
        ],
        compiler_params=pltpu.CompilerParams(
            collective_id=0, has_side_effects=True, vmem_limit_bytes=60 * 1024 * 1024
        ),
    )(
        queries,
        step_token_keys,
        step_token_values,
        stored_key_cache,
        stored_value_cache,
        lengths,
        gain_sides,
        resid,
        actions,
        wo_sides,
        head.T,
    )


def on_device(*args):
    queries, lengths, head = args[0], args[5], args[8]
    n = lax.axis_size("grp") * lax.axis_size("tp")
    width = queries.shape[2]
    group = QUERY_HEADS // KEY_VALUE_HEADS
    whole_heads = width % HEAD_SIZE == 0 and group % (width // HEAD_SIZE) == 0
    fits = lax.axis_size("role") == 2 and n % 2 == 0 and lengths.shape[0] == 8
    if whole_heads and fits and head.shape[0] == n * width and head.shape[1] > TILE:
        return fused(*args)
    return plain(*args)


def solution(mesh):
    in_specs = (
        P(None, None, ("grp", "tp")),
        P(),
        P(),
        P(None, ("grp", "tp"), None),
        P(None, ("grp", "tp"), None),
        P(),
        P("role", ("grp", "tp"), None),
        P("role", ("grp", "tp")),
        P(None, ("grp", "tp")),
        P(None, None, ("grp", "tp")),
        P(),
    )
    out_specs = (P("role", None), P("role", None, ("grp", "tp")))
    return jax.shard_map(
        on_device, mesh=mesh, in_specs=in_specs, out_specs=out_specs, check_vma=False
    )
```

```python
import functools
import math

import jax
import jax.numpy as jnp
from jax import lax
from jax.experimental import pallas as pl
from jax.experimental.pallas import tpu as pltpu
from jax.sharding import PartitionSpec as P

D = 8192
QUERY_HEADS = 64
KEY_VALUE_HEADS = 8
HEAD_SIZE = 128
DECODE_STEPS = 2


def swap_sides(value):
    return lax.ppermute(value, "role", [(0, 1), (1, 0)])


def plain(
    queries,
    step_token_keys,
    step_token_values,
    stored_key_cache,
    stored_value_cache,
    lengths,
    wo_sides,
    gain_sides,
    head,
    resid,
    actions,
):
    both = ("grp", "tp")
    place = lax.axis_index(both)
    step = 1 - lax.axis_index("role")
    count_of_rows = lengths.shape[0]
    shard_length = stored_key_cache.shape[1]
    query_group_width = QUERY_HEADS // KEY_VALUE_HEADS
    logit_scale = 1.0 / math.sqrt(HEAD_SIZE)
    query_matrix = lax.all_gather(
        lax.dynamic_index_in_dim(queries, step, 0, keepdims=False), both, axis=1, tiled=True
    )
    positions = place * shard_length + jnp.arange(shard_length, dtype=jnp.int32)
    valid = positions[None, :] < lengths[:, None]
    masking = valid[:, None, None, :]
    cache_shape = (count_of_rows, shard_length, KEY_VALUE_HEADS, HEAD_SIZE)
    prior_keys = stored_key_cache.reshape(cache_shape)
    prior_values = stored_value_cache.reshape(cache_shape)
    step_shape = (DECODE_STEPS, count_of_rows, KEY_VALUE_HEADS, HEAD_SIZE)
    incoming_keys = step_token_keys.astype(jnp.float32).reshape(step_shape)
    incoming_values = step_token_values.astype(jnp.float32).reshape(step_shape)
    current_query = query_matrix.reshape(
        count_of_rows, KEY_VALUE_HEADS, query_group_width, HEAD_SIZE
    )
    scores = (
        jnp.einsum("rkgd,rskd->rkgs", current_query, prior_keys, preferred_element_type=jnp.float32)
        * logit_scale
    )
    scores = jnp.where(masking, scores, -1e30)
    fresh_live = jnp.arange(DECODE_STEPS, dtype=jnp.int32) <= step
    fresh_scores = (
        jnp.einsum("rkgd,trkd->rkgt", current_query.astype(jnp.float32), incoming_keys)
        * logit_scale
    )
    fresh_scores = jnp.where(fresh_live, fresh_scores, -1e30)
    fresh_highest = jnp.max(fresh_scores, axis=-1)
    overall = lax.pmax(jnp.maximum(jnp.max(scores, axis=-1), fresh_highest), both)
    cache_probs = jnp.exp(scores - overall[..., None]) * masking
    fresh_probs = jnp.exp(fresh_scores - overall[..., None]) * fresh_live
    fresh_probs = fresh_probs * (place == 0)
    totals = jnp.sum(cache_probs, axis=-1) + jnp.sum(fresh_probs, axis=-1)
    weighted = jnp.einsum(
        "rkgs,rskd->rkgd", cache_probs, prior_values.astype(jnp.float32)
    ) + jnp.einsum("rkgt,trkd->rkgd", fresh_probs, incoming_values)
    features = QUERY_HEADS * HEAD_SIZE
    mixed = lax.psum_scatter(
        weighted.reshape(count_of_rows, features), both, scatter_dimension=1, tiled=True
    )
    totals = lax.psum(totals.reshape(count_of_rows, QUERY_HEADS), both)
    feature_rows = wo_sides.shape[1]
    own_heads = (place * feature_rows + jnp.arange(feature_rows)) // HEAD_SIZE
    own_part = (mixed / jnp.take(totals, own_heads, axis=1)).astype(jnp.bfloat16)
    branch_out = lax.psum_scatter(
        jnp.dot(own_part, wo_sides[0], preferred_element_type=jnp.float32),
        both,
        scatter_dimension=1,
        tiled=True,
    )
    resid_now = lax.dynamic_index_in_dim(resid, step, 0, keepdims=False)
    state = resid_now.astype(jnp.float32) + branch_out
    square_sum = lax.psum(jnp.sum(state * state, axis=-1), both)
    normed_now = (
        state * lax.rsqrt(square_sum[:, None] / D + 1e-05) * gain_sides[0][None, :]
    ).astype(jnp.bfloat16)
    logits = jnp.dot(
        lax.all_gather(normed_now, both, axis=1, tiled=True),
        head,
        preferred_element_type=jnp.float32,
    )
    local_highest = jnp.max(logits, axis=-1)
    action_now = lax.dynamic_index_in_dim(actions, step, 0, keepdims=False)
    head_width = head.shape[1]
    vocab_ids = place * head_width + jnp.arange(head_width, dtype=jnp.int32)
    is_target = vocab_ids[None, :] == action_now[:, None]
    target = jnp.sum(jnp.where(is_target, logits, 0.0), axis=-1)
    exp_sum = jnp.sum(jnp.exp(logits - local_highest[:, None]), axis=-1)
    parts = lax.all_gather(jnp.stack([local_highest, exp_sum, target]), both)
    largest = jnp.max(parts[:, 0], axis=0)
    exp_sum = jnp.sum(parts[:, 1] * jnp.exp(parts[:, 0] - largest[None]), axis=0)
    prob_now = jnp.sum(parts[:, 2], axis=0) - largest - jnp.log(exp_sum)
    return (swap_sides(prob_now)[None], swap_sides(normed_now)[None])


LOW = -1e30
TILE = 512
MESH = pl.DeviceIdType.MESH


def fused_kernel(
    n,
    tp,
    queries,
    token_keys,
    token_values,
    keys_in,
    values_in,
    lengths,
    gain,
    resid,
    actions,
    wo,
    head,
    log_probs,
    normed,
    keys,
    values,
    wo_buf,
    head_buf,
    q_all,
    b_send,
    b_recv,
    c_send,
    c_recv,
    d_send,
    d_recv,
    x_send,
    x_recv,
    s_send,
    s_recv,
    x_rows,
    y_keep,
    y_send,
    y_recv,
    e_send,
    e_recv,
    kv_sems,
    wo_sem,
    head_sems,
    q_ss,
    q_rs,
    b_ss,
    b_rs,
    c_ss,
    c_rs,
    d_ss,
    d_rs,
    x_sem,
    s_ss,
    s_rs,
    y_ss,
    y_rs,
    e_ss,
    e_rs,
):
    role = lax.axis_index("role")
    me = lax.axis_index("grp") * tp + lax.axis_index("tp")
    step = 1 - role
    half = n // 2
    rows = lengths.shape[0]
    shard = keys.shape[1]
    width = resid.shape[2]
    own_heads = width // HEAD_SIZE
    group = QUERY_HEADS // KEY_VALUE_HEADS
    slots = rows * shard
    depth = head_buf.shape[1]
    vocab = head.shape[0]
    full = vocab // TILE
    tail = vocab - full * TILE
    tiles = y_keep.shape[0]
    scale = 1.0 / math.sqrt(HEAD_SIZE)
    f32 = jnp.float32
    bf16 = jnp.bfloat16

    def device(side, place):
        return (side, place // tp, place % tp)

    def remote(src, dst, ss, rs, side, place):
        return pltpu.make_async_remote_copy(
            src_ref=src,
            dst_ref=dst,
            send_sem=ss,
            recv_sem=rs,
            device_id=device(side, place),
            device_id_type=MESH,
        )

    key_copy = pltpu.make_async_copy(keys_in, keys, kv_sems.at[0])
    value_copy = pltpu.make_async_copy(values_in, values, kv_sems.at[1])
    key_copy.start()
    value_copy.start()
    wo_copy = pltpu.make_async_copy(wo.at[0], wo_buf, wo_sem)
    wo_copy.start()

    def head_copy(first, size, sem):
        return pltpu.make_async_copy(
            head.at[pl.ds(first, size), pl.ds(pl.multiple_of(role * depth, 128), depth)],
            head_buf.at[pl.ds(first, size), :],
            sem,
        )

    @pl.loop(0, full)
    def _(j):
        head_copy(pl.multiple_of(j * TILE, TILE), TILE, head_sems.at[j]).start()

    if tail:
        head_copy(full * TILE, tail, head_sems.at[full]).start()

    barrier = pltpu.get_barrier_semaphore()

    @pl.loop(1, 2 * n)
    def _(i):
        other = (role * n + me + i) % (2 * n)
        pl.semaphore_signal(
            barrier, inc=1, device_id=device(other // n, other % n), device_id_type=MESH
        )

    pl.semaphore_wait(barrier, 2 * n - 1)

    @pl.loop(1, n)
    def _(i):
        to = (me + i) % n
        remote(queries.at[step], q_all.at[me], q_ss.at[i], q_rs.at[me], role, to).start()

    q_all[me] = queries[step]

    row_ids = lax.broadcasted_iota(jnp.int32, (group * rows, slots), 0) % rows
    col_ids = lax.broadcasted_iota(jnp.int32, (group * rows, slots), 1)
    limit = jnp.zeros((group * rows, slots), jnp.int32)
    for b in range(rows):
        limit = jnp.where(row_ids == b, lengths[b], limit)
    place_ids = me * shard + col_ids % shard
    live = (col_ids // shard == row_ids) & (place_ids < limit)

    @pl.loop(1, n)
    def _(i):
        src = (me + i) % n
        remote(queries.at[step], q_all.at[src], q_ss.at[i], q_rs.at[src], role, me).wait_recv()

    key_copy.wait()
    value_copy.wait()

    lane = lax.broadcasted_iota(jnp.int32, (rows, HEAD_SIZE), 1)
    per_group = group // own_heads
    for k in range(KEY_VALUE_HEADS):
        lanes = slice(k * HEAD_SIZE, (k + 1) * HEAD_SIZE)
        query = jnp.concatenate(
            [
                q_all[
                    k * per_group + h // own_heads,
                    :,
                    (h % own_heads) * HEAD_SIZE : (h % own_heads + 1) * HEAD_SIZE,
                ].astype(f32)
                for h in range(group)
            ],
            axis=0,
        ).astype(bf16)
        key = keys[:, :, lanes].reshape(slots, HEAD_SIZE)
        value = values[:, :, lanes].reshape(slots, HEAD_SIZE)
        scores = (
            lax.dot_general(query, key, (((1,), (1,)), ((), ())), preferred_element_type=f32)
            * scale
        )
        scores = jnp.where(live, scores, LOW)
        top = jnp.max(scores, axis=1, keepdims=True).astype(bf16).astype(f32)
        probs = jnp.where(live, jnp.exp(scores - top), 0.0).astype(bf16)
        total = jnp.sum(probs.astype(f32), axis=1, keepdims=True)
        total_high = total.astype(bf16).astype(f32)
        total_low = total - total_high
        weighted = jnp.dot(probs, value, preferred_element_type=f32)
        for part in range(per_group):
            to = k * per_group + part
            stats = jnp.zeros((rows, HEAD_SIZE), f32)
            for j in range(own_heads):
                at = (part * own_heads + j) * rows
                stats = jnp.where(lane == j, top[at : at + rows], stats)
                stats = jnp.where(lane == own_heads + j, total_high[at : at + rows], stats)
                stats = jnp.where(lane == 2 * own_heads + j, total_low[at : at + rows], stats)
            first = part * own_heads * rows
            b_send[to] = jnp.concatenate(
                [weighted[first : first + own_heads * rows], stats, jnp.zeros_like(stats)], axis=0
            ).astype(bf16)

    @pl.loop(1, n)
    def _(i):
        to = (me + i) % n
        remote(b_send.at[to], b_recv.at[me], b_ss.at[i], b_rs.at[me], role, to).start()

    b_recv[me] = b_send[me]

    kv_lanes = pl.ds(pl.multiple_of((me // per_group) * HEAD_SIZE, HEAD_SIZE), HEAD_SIZE)
    own_query = queries[step].astype(f32)
    fresh = []
    fresh_values = []
    for u in range(DECODE_STEPS):
        fresh_key = token_keys[u, :, kv_lanes].astype(f32)
        fresh_values.append(token_values[u, :, kv_lanes].astype(f32))
        fresh.append(
            [
                jnp.where(
                    u <= step,
                    jnp.sum(
                        own_query[:, j * HEAD_SIZE : (j + 1) * HEAD_SIZE] * fresh_key,
                        axis=1,
                        keepdims=True,
                    )
                    * scale,
                    LOW,
                )
                for j in range(own_heads)
            ]
        )

    @pl.loop(1, n)
    def _(i):
        src = (me + i) % n
        remote(b_send.at[src], b_recv.at[src], b_ss.at[i], b_rs.at[src], role, me).wait_recv()

    stat_rows = slice(own_heads * rows, own_heads * rows + 16)
    stats = [b_recv[s, stat_rows, :].astype(f32)[:rows] for s in range(n)]
    top = functools.reduce(jnp.maximum, stats)
    tops = [
        functools.reduce(
            jnp.maximum, [fresh[u][j] for u in range(DECODE_STEPS)], top[:, j : j + 1]
        )
        for j in range(own_heads)
    ]
    numerator = [jnp.zeros((rows, HEAD_SIZE), f32) for _ in range(own_heads)]
    denominator = [jnp.zeros((rows, 1), f32) for _ in range(own_heads)]
    for j in range(own_heads):
        for u in range(DECODE_STEPS):
            weight = jnp.where(u <= step, jnp.exp(fresh[u][j] - tops[j]), 0.0)
            numerator[j] += weight * fresh_values[u]
            denominator[j] += weight
    for s in range(n):
        part = b_recv[s, : own_heads * rows, :].astype(f32)
        for j in range(own_heads):
            factor = jnp.exp(stats[s][:, j : j + 1] - tops[j])
            numerator[j] += factor * part[j * rows : (j + 1) * rows]
            at = own_heads + j
            denominator[j] += factor * (
                stats[s][:, at : at + 1] + stats[s][:, at + own_heads : at + own_heads + 1]
            )
    attended = jnp.concatenate(
        [numerator[j] / denominator[j] for j in range(own_heads)], axis=1
    ).astype(bf16)

    wo_copy.wait()

    def project(to):
        return jnp.dot(
            attended,
            wo_buf[:, pl.ds(pl.multiple_of(to * width, 128), width)],
            preferred_element_type=f32,
        )

    @pl.loop(1, n)
    def _(i):
        to = (me + i) % n
        c_send[to] = project(to).astype(bf16)
        remote(c_send.at[to], c_recv.at[me], c_ss.at[i], c_rs.at[me], role, to).start()

    c_recv[me] = jnp.zeros((rows, width), bf16)
    state = resid[step].astype(f32) + project(me)

    @pl.loop(1, n)
    def _(i):
        src = (me + i) % n
        remote(c_send.at[src], c_recv.at[src], c_ss.at[i], c_rs.at[src], role, me).wait_recv()

    for s in range(n):
        state += c_recv[s].astype(f32)

    x = state * gain[...]
    d_send[...] = x.astype(bf16)
    x_send[...] = x
    s_send[...] = jnp.broadcast_to(jnp.sum(state * state, axis=1, keepdims=True), (rows, HEAD_SIZE))
    target_role = me // half
    own_slot = role * half + me % half

    @pl.when(target_role != role)
    def _():
        remote(
            d_send, d_recv.at[own_slot], d_ss.at[0], d_rs.at[own_slot], target_role, me
        ).start()

    @pl.when(target_role == role)
    def _():
        d_recv[own_slot] = d_send[...]

    @pl.loop(1, n)
    def _(i):
        to = (me + i) % n
        remote(
            d_send, d_recv.at[own_slot], d_ss.at[i], d_rs.at[own_slot], target_role, to
        ).start()

    @pl.loop(0, n)
    def _(i):
        to = (me + i) % n
        remote(s_send, s_recv.at[me], s_ss.at[i], s_rs.at[me], 1 - role, to).start()

    remote(x_send, x_recv, x_sem.at[0], x_sem.at[1], 1 - role, me).start()

    @pl.loop(0, n)
    def _(slot):
        mine = (slot // half == role) & (role * half + slot % half == me)

        @pl.when(jnp.logical_not(mine))
        def _():
            remote(d_send, d_recv.at[slot], d_ss.at[0], d_rs.at[slot], role, me).wait_recv()

    for f in range(half):
        x_rows[:, f * width : (f + 1) * width] = jnp.concatenate(
            [d_recv[half + f].astype(f32), d_recv[f].astype(f32)], axis=0
        ).astype(bf16)

    def vocab_dot(block):
        return lax.dot_general(
            x_rows[...], block, (((1,), (1,)), ((), ())), preferred_element_type=f32
        )

    def y_copy(j):
        return remote(y_send.at[j], y_recv.at[j], y_ss.at[j], y_rs.at[j], 1 - role, me)

    @pl.loop(0, full)
    def _(j):
        first = pl.multiple_of(j * TILE, TILE)
        head_copy(first, TILE, head_sems.at[j]).wait()
        y = vocab_dot(head_buf[pl.ds(first, TILE), :])
        y_keep[j] = jnp.where(role == 0, y[:rows], y[rows:])
        y_send[j] = jnp.where(role == 0, y[rows:], y[:rows])
        y_copy(j).start()

    if tail:
        head_copy(full * TILE, tail, head_sems.at[full]).wait()
        y = vocab_dot(head_buf[full * TILE :, :])
        y_keep[full] = jnp.zeros((rows, TILE), f32)
        y_send[full] = jnp.zeros((rows, TILE), f32)
        y_keep[full, :, :tail] = jnp.where(role == 0, y[:rows], y[rows:])
        y_send[full, :, :tail] = jnp.where(role == 0, y[rows:], y[:rows])
        y_copy(full).start()

    @pl.loop(0, n)
    def _(s):
        remote(s_send, s_recv.at[s], s_ss.at[s], s_rs.at[s], role, me).wait_recv()

    square_sum = jnp.zeros((rows, HEAD_SIZE), f32)
    for s in range(n):
        square_sum += s_recv[s]
    inverse = lax.rsqrt(square_sum / (n * width) + 1e-05)[:, :1]
    remote(x_send, x_recv, x_sem.at[0], x_sem.at[1], role, me).wait_recv()
    normed[0] = (x_recv[...] * inverse).astype(bf16)

    action_rows = lax.broadcasted_iota(jnp.int32, (rows, 1), 0)
    action = jnp.zeros((rows, 1), jnp.int32)
    for b in range(rows):
        action = jnp.where(action_rows == b, actions[role, b], action)
    tile_ids = lax.broadcasted_iota(jnp.int32, (rows, TILE), 1)
    logits = []
    for j in range(tiles):
        y_copy(j).wait_recv()
        tile = (y_keep[j] + y_recv[j]) * inverse
        if j == full:
            tile = jnp.where(tile_ids < tail, tile, LOW)
        logits.append(tile)
    largest = jnp.max(functools.reduce(jnp.maximum, logits), axis=1, keepdims=True)
    exp_sum = jnp.zeros((rows, TILE), f32)
    target = jnp.zeros((rows, TILE), f32)
    for j in range(tiles):
        exp_sum += jnp.exp(logits[j] - largest)
        here = tile_ids + j * TILE == action - me * vocab
        if j == full:
            here = here & (tile_ids < tail)
        target += jnp.where(here, logits[j], 0.0)
    exp_sum = jnp.sum(exp_sum, axis=1, keepdims=True)
    target = jnp.sum(target, axis=1, keepdims=True)
    e_send[...] = jnp.where(lane == 0, largest, jnp.where(lane == 1, exp_sum, target))

    @pl.loop(1, n)
    def _(i):
        to = (me + i) % n
        remote(e_send, e_recv.at[me], e_ss.at[i], e_rs.at[me], role, to).start()

    e_recv[me] = e_send[...]

    @pl.loop(1, n)
    def _(i):
        src = (me + i) % n
        remote(e_send, e_recv.at[src], e_ss.at[i], e_rs.at[src], role, me).wait_recv()

    top = functools.reduce(jnp.maximum, [e_recv[s] for s in range(n)])[:, :1]
    exp_sum = jnp.zeros((rows, 1), f32)
    target = jnp.zeros((rows, 1), f32)
    for s in range(n):
        got = e_recv[s]
        exp_sum += got[:, 1:2] * jnp.exp(got[:, :1] - top)
        target += got[:, 2:3]
    result = jnp.broadcast_to(target - top - jnp.log(exp_sum), (rows, HEAD_SIZE))
    diagonal = lax.broadcasted_iota(jnp.int32, (rows, HEAD_SIZE), 0) == lane
    log_probs[...] = jnp.sum(jnp.where(diagonal, result, 0.0), axis=0, keepdims=True)[:, :rows]

    @pl.loop(1, n)
    def _(i):
        to = (me + i) % n
        remote(queries.at[step], q_all.at[me], q_ss.at[i], q_rs.at[me], role, to).wait_send()
        remote(b_send.at[to], b_recv.at[me], b_ss.at[i], b_rs.at[me], role, to).wait_send()
        remote(c_send.at[to], c_recv.at[me], c_ss.at[i], c_rs.at[me], role, to).wait_send()
        remote(
            d_send, d_recv.at[own_slot], d_ss.at[i], d_rs.at[own_slot], target_role, to
        ).wait_send()
        remote(e_send, e_recv.at[me], e_ss.at[i], e_rs.at[me], role, to).wait_send()

    @pl.when(target_role != role)
    def _():
        remote(
            d_send, d_recv.at[own_slot], d_ss.at[0], d_rs.at[own_slot], target_role, me
        ).wait_send()

    @pl.loop(0, n)
    def _(i):
        remote(s_send, s_recv.at[me], s_ss.at[i], s_rs.at[me], 1 - role, me).wait_send()

    remote(x_send, x_recv, x_sem.at[0], x_sem.at[1], 1 - role, me).wait_send()
    for j in range(tiles):
        y_copy(j).wait_send()


def fused(
    queries,
    step_token_keys,
    step_token_values,
    stored_key_cache,
    stored_value_cache,
    lengths,
    wo_sides,
    gain_sides,
    head,
    resid,
    actions,
):
    tp = lax.axis_size("tp")
    n = lax.axis_size("grp") * tp
    rows = lengths.shape[0]
    width = resid.shape[2]
    heads = width // HEAD_SIZE
    depth = head.shape[0] // 2
    tiles = -(-head.shape[1] // TILE)
    bf16, f32 = jnp.bfloat16, jnp.float32
    vmem = pl.BlockSpec(memory_space=pltpu.VMEM)
    smem = pl.BlockSpec(memory_space=pltpu.SMEM)
    hbm = pl.BlockSpec(memory_space=pl.ANY)
    message = heads * rows + 2 * rows
    dma = pltpu.SemaphoreType.DMA
    return pl.pallas_call(
        functools.partial(fused_kernel, n, tp),
        out_shape=(
            jax.ShapeDtypeStruct((1, rows), f32),
            jax.ShapeDtypeStruct((1, rows, width), bf16),
        ),
        in_specs=[vmem, vmem, vmem, hbm, hbm, smem, vmem, vmem, smem, hbm, hbm],
        out_specs=(vmem, vmem),
        scratch_shapes=[
            pltpu.VMEM(stored_key_cache.shape, bf16),
            pltpu.VMEM(stored_value_cache.shape, bf16),
            pltpu.VMEM(wo_sides.shape[1:], bf16),
            pltpu.VMEM((head.shape[1], depth), bf16),
            pltpu.VMEM((n, rows, width), bf16),
            pltpu.VMEM((n, message, HEAD_SIZE), bf16),
            pltpu.VMEM((n, message, HEAD_SIZE), bf16),
            pltpu.VMEM((n, rows, width), bf16),
            pltpu.VMEM((n, rows, width), bf16),
            pltpu.VMEM((rows, width), bf16),
            pltpu.VMEM((n, rows, width), bf16),
            pltpu.VMEM((rows, width), f32),
            pltpu.VMEM((rows, width), f32),
            pltpu.VMEM((rows, HEAD_SIZE), f32),
            pltpu.VMEM((n, rows, HEAD_SIZE), f32),
            pltpu.VMEM((2 * rows, depth), bf16),
            pltpu.VMEM((tiles, rows, TILE), f32),
            pltpu.VMEM((tiles, rows, TILE), f32),
            pltpu.VMEM((tiles, rows, TILE), f32),
            pltpu.VMEM((rows, HEAD_SIZE), f32),
            pltpu.VMEM((n, rows, HEAD_SIZE), f32),
            dma((2,)),
            dma,
            dma((tiles,)),
            dma((n,)),
            dma((n,)),
            dma((n,)),
            dma((n,)),
            dma((n,)),
            dma((n,)),
            dma((n,)),
            dma((n,)),
            dma((2,)),
            dma((n,)),
            dma((n,)),
            dma((tiles,)),
            dma((tiles,)),
            dma((n,)),
            dma((n,)),
        ],
        compiler_params=pltpu.CompilerParams(
            collective_id=0, has_side_effects=True, vmem_limit_bytes=60 * 1024 * 1024
        ),
    )(
        queries,
        step_token_keys,
        step_token_values,
        stored_key_cache,
        stored_value_cache,
        lengths,
        gain_sides,
        resid,
        actions,
        wo_sides,
        head.T,
    )


def on_device(*args):
    queries, lengths, head = args[0], args[5], args[8]
    n = lax.axis_size("grp") * lax.axis_size("tp")
    width = queries.shape[2]
    group = QUERY_HEADS // KEY_VALUE_HEADS
    whole_heads = width % HEAD_SIZE == 0 and group % (width // HEAD_SIZE) == 0
    fits = lax.axis_size("role") == 2 and n % 2 == 0 and lengths.shape[0] == 8
    if whole_heads and fits and head.shape[0] == n * width and head.shape[1] > TILE:
        return fused(*args)
    return plain(*args)


def solution(mesh):
    in_specs = (
        P(None, None, ("grp", "tp")),
        P(),
        P(),
        P(None, ("grp", "tp"), None),
        P(None, ("grp", "tp"), None),
        P(),
        P("role", ("grp", "tp"), None),
        P("role", ("grp", "tp")),
        P(None, ("grp", "tp")),
        P(None, None, ("grp", "tp")),
        P(),
    )
    out_specs = (P("role", None), P("role", None, ("grp", "tp")))
    return jax.shard_map(
        on_device, mesh=mesh, in_specs=in_specs, out_specs=out_specs, check_vma=False
    )
```
